8 devices in a mesh: dp: 2 (over y, z), tp: 4 (over x, core).
Axes of the slice: x: 2, y: 2, z: 1, core: 2. Of those that a mesh axis runs over, the one named last changes fastest.
Arguments:
- x: bfloat16 [128, 3072], P('dp'), parts along dimension 0
- k_cache: bfloat16 [128, 4096, 8, 128], P('dp', None, 'tp'), parts along dimension 0
- v_cache: bfloat16 [128, 4096, 8, 128], P('dp', None, 'tp'), parts along dimension 0
- gain_a: bfloat16 [3072], replicated
- wq: bfloat16 [3072, 3072], P(None, 'tp')
- wo: bfloat16 [3072, 3072], P('tp')
- gain_m: bfloat16 [3072], replicated
- w_gate: bfloat16 [3072, 8192], P(None, 'tp')
- w_up: bfloat16 [3072, 8192], P(None, 'tp')
- w_down: bfloat16 [8192, 3072], P('tp')
Outputs:
- output: bfloat16 [128, 3072], P('dp'), parts along dimension 0
There are 2 independent parts. The reference program is written for one: setup_inputs(seed, part) draws one part's arguments, and reference() takes and returns one part's arrays. A program takes and returns all parts, laid end to end along the dimension named above; an argument that names none is the same for every part.
All inputs are finite; a program needn't handle non-finite values.
Results may differ from the reference program's by a relative error of at most 0.017.
Values are sent between devices in bfloat16 or wider.
A program may use at most 2 GiB of HBM per device.

```python
import jax
import jax.numpy as jnp
from jax import lax

BATCH = 64
CACHE = 4096
D = 3072
HEADS = 24
KV_HEADS = 8
HEAD = 128
FF = 8192
THETA = 10000


def setup_inputs(seed: int = 0, part: int = 0) -> dict:
    kx, kc, kw, kn, kq, ko, km, kg, ku, kd = jax.random.split(jax.random.key(seed), 10)
    kx, kc, kw = (jax.random.fold_in(k, part) for k in (kx, kc, kw))

    def weights(key, rows, columns):
        return jax.random.normal(key, (rows, columns), jnp.float32) * rows**-0.5

    drawn = {
        "x": jax.random.normal(kx, (BATCH, D), jnp.float32),
        "k_cache": 2 * jax.random.normal(kc, (BATCH, CACHE, KV_HEADS, HEAD), jnp.float32),
        "v_cache": 4 * jax.random.normal(kw, (BATCH, CACHE, KV_HEADS, HEAD), jnp.float32),
        "gain_a": 1 + 0.1 * jax.random.normal(kn, (D,), jnp.float32),
        "wq": 2 * weights(kq, D, HEADS * HEAD),
        "wo": weights(ko, HEADS * HEAD, D),
        "gain_m": 1 + 0.1 * jax.random.normal(km, (D,), jnp.float32),
        "w_gate": weights(kg, D, FF),
        "w_up": weights(ku, D, FF),
        "w_down": 2 * weights(kd, FF, D),
    }
    return {k: v.astype(jnp.bfloat16) for k, v in drawn.items()}


def normed(x, gain):
    wide = x.astype(jnp.float32)
    scale = lax.rsqrt(jnp.mean(wide * wide, -1, keepdims=True) + 1e-6)
    return (wide * scale * gain.astype(jnp.float32)).astype(jnp.bfloat16)


def turned(t, place, theta):
    half = t.shape[-1] // 2
    angle = place.astype(jnp.float32)[:, None] * theta ** (-jnp.arange(half, dtype=jnp.float32) / half)
    cos, sin = jnp.cos(angle)[:, None], jnp.sin(angle)[:, None]
    a, b = t[..., :half].astype(jnp.float32), t[..., half:].astype(jnp.float32)
    return jnp.concatenate([a * cos - b * sin, b * cos + a * sin], -1).astype(jnp.bfloat16)


def matmul(a, w):
    return jnp.dot(a, w, preferred_element_type=jnp.float32).astype(jnp.bfloat16)


def einsum(form, a, b):
    return jnp.einsum(form, a.astype(jnp.float32), b.astype(jnp.float32))


def seen_by(a, wq, k_cache, v_cache, head, theta):
    batch, cache, kv_heads = k_cache.shape[:3]
    place = jnp.full((batch,), cache - 1)
    q = turned(matmul(a, wq).reshape(batch, -1, head), place, theta).reshape(batch, kv_heads, -1, head)
    scores = einsum("bgsd,bugd->bgsu", q, k_cache) * head**-0.5
    weights = jax.nn.softmax(scores, -1).astype(jnp.bfloat16)
    return einsum("bgsu,bugd->bgsd", weights, v_cache).astype(jnp.bfloat16).reshape(batch, -1)


def hidden_of(b, w_gate, w_up):
    gate = jnp.dot(b, w_gate, preferred_element_type=jnp.float32)
    up = jnp.dot(b, w_up, preferred_element_type=jnp.float32)
    return (jax.nn.silu(gate) * up).astype(jnp.bfloat16)


def reference(x, k_cache, v_cache, gain_a, wq, wo, gain_m, w_gate, w_up, w_down):
    seen = seen_by(normed(x, gain_a), wq, k_cache, v_cache, HEAD, THETA)
    h = (x.astype(jnp.float32) + jnp.dot(seen, wo, preferred_element_type=jnp.float32)).astype(jnp.bfloat16)
    hidden = hidden_of(normed(h, gain_m), w_gate, w_up)
    return (h.astype(jnp.float32) + jnp.dot(hidden, w_down, preferred_element_type=jnp.float32)).astype(jnp.bfloat16)
```

```python
import functools

import jax
import jax.numpy as jnp
import numpy as np
from jax import lax
from jax.experimental import pallas as pl
from jax.experimental.pallas import tpu as pltpu
from jax.sharding import PartitionSpec as P

MESH = pl.DeviceIdType.MESH
BF16, F32 = jnp.bfloat16, jnp.float32
HEAD = 128
THETA = 10000
SEQS, CACHE, D, FF = 64, 4096, 3072, 2048
HEADS, KV = 6, 2
RING = 4
CHUNK = 512
COLS = 512
HALF = D // 2
BLOCKS = HALF // COLS
FF_BLOCKS = FF // COLS


def dot(a, w):
    return jnp.dot(a, w, preferred_element_type=F32)


def normed(x, gain):
    wide = x.astype(F32)
    scale = lax.rsqrt(jnp.mean(wide * wide, -1, keepdims=True) + 1e-6)
    return (wide * scale * gain.astype(F32)).astype(BF16)


def pair(ref, p, first, rows):
    at = 2 * p * CHUNK + first
    return jnp.concatenate([ref[at : at + rows, :], ref[at + CHUNK : at + CHUNK + rows, :]], 1)


def scores_of(k, q):
    zero = jnp.zeros((8, HEAD), F32)
    two = jnp.concatenate([jnp.concatenate([q, zero], 1), jnp.concatenate([zero, q], 1)], 0).astype(BF16)
    sums = [None, None]
    rows = CHUNK // 2
    for p in range(8):
        above, below = [jnp.zeros((n, 2 * HEAD), BF16) for n in (16 * p, 112 - 16 * p)]
        spread = jnp.concatenate([*([above] if p else []), two, *([below] if p < 7 else [])], 0)
        for h in range(2):
            term = lax.dot_general(pair(k, p, h * rows, rows), spread, (((1,), (1,)), ((), ())), preferred_element_type=F32)
            sums[h] = term if sums[h] is None else sums[h] + term
    return jnp.concatenate(sums, 0).T


def attended(scores, v, seen):
    s = scores.reshape(16, 8, CHUNK)
    s = jnp.where(seen, s, -jnp.inf)
    top = jnp.max(jnp.max(s, 0), 1, keepdims=True)
    e = jnp.exp2((s - top[None]) * (HEAD**-0.5 * 1.4426950408889634))
    total = jnp.sum(jnp.sum(e, 0), 1, keepdims=True)
    w = (e * (1.0 / total)[None]).reshape(128, CHUNK).astype(BF16)
    sums = [None, None]
    rows = CHUNK // 2
    for p in range(8):
        for h in range(2):
            term = dot(w[16 * p : 16 * p + 16, h * rows : h * rows + rows], pair(v, p, h * rows, rows))
            sums[h] = term if sums[h] is None else sums[h] + term
    both = sums[0] + sums[1]
    return both[:8, :HEAD] + both[8:, HEAD:]


def kernel(
    x_hbm, k_hbm, v_hbm, ga_hbm, wq_hbm, wo_hbm, gm_hbm, wg_hbm, wu_hbm, wd_hbm, turn_hbm,
    y_hbm,
    x, ga, gm, turn, kbuf, vbuf, wo, wg, wu, wd, q, o, scores, h, hidden, y,
    half_out, half_in, chip_out, chip_in,
    ksem, vsem, small_sem, wq_sem, wo_sem, wg_sem, wu_sem, wd_sem, y_sem, send_sem, recv_sem,
):
    me = lax.axis_index("tp")
    core = lax.rem(me, 2)
    partner = me + 1 - 2 * core
    across = lax.rem(me + 2, 4)
    own, other = core * HALF, (1 - core) * HALF

    def columns(start, i):
        return pl.ds(pl.multiple_of(start + i * COLS, COLS), COLS)

    small = [
        pltpu.make_async_copy(a, b, small_sem.at[i])
        for i, (a, b) in enumerate(((x_hbm, x), (ga_hbm, ga), (gm_hbm, gm), (turn_hbm, turn)))
    ]
    wq_copies = [
        pltpu.make_async_copy(wq_hbm.at[:, 0:512], wg.at[2], wq_sem.at[0]),
        pltpu.make_async_copy(wq_hbm.at[:, 512:768], wg.at[3, :, 0:256], wq_sem.at[1]),
    ]

    def k_copy(t):
        return pltpu.make_async_copy(k_hbm.at[t], kbuf.at[lax.rem(t, RING)], ksem.at[lax.rem(t, RING)])

    def v_copy(t):
        return pltpu.make_async_copy(v_hbm.at[t], vbuf.at[lax.rem(t, RING)], vsem.at[lax.rem(t, RING)])

    wo_copies, wd_copies = [
        [
            pltpu.make_async_copy(hbm.at[:, columns(other if i < BLOCKS else own, i % BLOCKS)], buf.at[i], sem.at[i])
            for i in range(2 * BLOCKS)
        ]
        for hbm, buf, sem in ((wo_hbm, wo, wo_sem), (wd_hbm, wd, wd_sem))
    ]
    wg_copies, wu_copies = [
        [pltpu.make_async_copy(hbm.at[:, i * COLS : (i + 1) * COLS], buf.at[i], sem.at[i]) for i in range(FF_BLOCKS)]
        for hbm, buf, sem in ((wg_hbm, wg, wg_sem), (wu_hbm, wu, wu_sem))
    ]

    for c in (*small, *wq_copies):
        c.start()
    for t in range(RING):
        k_copy(jnp.int32(t)).start()
        v_copy(jnp.int32(t)).start()

    barrier = pltpu.get_barrier_semaphore()
    for d in (partner, across):
        pl.semaphore_signal(barrier, inc=1, device_id={"tp": d}, device_id_type=MESH)

    for c in small:
        c.wait()
    a = normed(x[...], ga[...])
    for c in wq_copies:
        c.wait()
    projected = jnp.concatenate([dot(a, wg[2]), dot(a, wg[3, :, 0:256])], 1).astype(BF16).astype(F32)
    cos, sin = turn[0:1, :], turn[1:2, :]
    for i in range(HEADS):
        t = projected[:, i * HEAD : (i + 1) * HEAD]
        q[:, i, :] = (t * cos + pltpu.roll(t, HEAD // 2, 1) * sin).astype(BF16).astype(F32)
    for i in range(HEADS, 8):
        q[:, i, :] = jnp.zeros((SEQS, HEAD), F32)

    row = lax.broadcasted_iota(jnp.int32, (8, CHUNK), 0)
    odd = lax.broadcasted_iota(jnp.int32, (8, CHUNK), 1) % 2
    seen = (((row < 3) & (odd == 0)) | ((row >= 3) & (row < 6) & (odd == 1)) | (row >= 6))[None]

    first = jnp.int32(0)
    k_copy(first).wait()
    scores[...] = scores_of(kbuf.at[0], q[0])
    k_copy(first + RING).start()

    def step(t, _):
        k_copy(t + 1).wait()
        v_copy(t).wait()
        before = scores[...]
        after = scores_of(kbuf.at[lax.rem(t + 1, RING)], q[t + 1])
        o[t] = attended(before, vbuf.at[lax.rem(t, RING)], seen)
        scores[...] = after

        @pl.when(t + RING < SEQS)
        def _():
            v_copy(t + RING).start()

            @pl.when(t + 1 + RING < SEQS)
            def _():
                k_copy(t + 1 + RING).start()

        @pl.when(t == SEQS - RING)
        def _():
            for c in (*wo_copies, *(c for two in zip(wg_copies, wu_copies) for c in two), *wd_copies):
                c.start()

        return 0

    lax.fori_loop(0, SEQS - 1, step, 0)
    last = jnp.int32(SEQS - 1)
    v_copy(last).wait()
    o[SEQS - 1] = attended(scores[...], vbuf.at[RING - 1], seen)

    pl.semaphore_wait(barrier, 2)

    def added(which, lhs, w, w_copies, base, out, out_other, keep):
        def remote(phase, i, src, dst, device):
            return pltpu.make_async_remote_copy(
                src_ref=src, dst_ref=dst, send_sem=send_sem.at[which, phase, i], recv_sem=recv_sem.at[which, phase, i],
                device_id={"tp": device}, device_id_type=MESH,
            )

        halves = [remote(0, i, half_out.at[which, i], half_in.at[which, i], partner) for i in range(BLOCKS)]
        chips = [remote(1, i, chip_out.at[which, i], chip_in.at[which, i], across) for i in range(BLOCKS)]
        finals = [remote(2, i, out.at[:, columns(own, i)], out_other.at[:, columns(own, i)], partner) for i in range(BLOCKS)]
        for i in range(BLOCKS):
            w_copies[i].wait()
            half_out[which, i] = dot(lhs, w[i]).astype(BF16)
            halves[i].start()
        for i in range(BLOCKS):
            w_copies[BLOCKS + i].wait()
            term = dot(lhs, w[BLOCKS + i])
            halves[i].wait_recv()
            chip_out[which, i] = (term + half_in[which, i].astype(F32)).astype(BF16)
            chips[i].start()
        for i in range(BLOCKS):
            chips[i].wait_recv()
            total = chip_out[which, i].astype(F32) + chip_in[which, i].astype(F32)
            out[:, columns(own, i)] = (base[:, columns(own, i)].astype(F32) + total).astype(BF16)
            finals[i].start()
            keep(i)
        for c in finals:
            c.wait()
        for c in (*halves, *chips):
            c.wait_send()

    attention = jnp.concatenate([o[:, i, :] for i in range(HEADS)], 1).astype(BF16)
    added(0, attention, wo, wo_copies, x, h, h, lambda i: None)

    b = normed(h[...], gm[...])
    for i in range(FF_BLOCKS):
        wg_copies[i].wait()
        wu_copies[i].wait()
        gate = dot(b, wg[i])
        up = dot(b, wu[i])
        hidden[:, i * COLS : (i + 1) * COLS] = (gate * lax.logistic(gate) * up).astype(BF16)

    y_copies = [
        pltpu.make_async_copy(y.at[:, columns(own, i)], y_hbm.at[:, columns(own, i)], y_sem.at[i]) for i in range(BLOCKS)
    ]
    added(1, hidden[...], wd, wd_copies, h, y, y_hbm, lambda i: y_copies[i].start())
    for c in y_copies:
        c.wait()


def layer(x, k_cache, v_cache, gain_a, wq, wo, gain_m, w_gate, w_up, w_down):
    half = HEAD // 2
    angle = np.float32(CACHE - 1) * np.float32(THETA) ** (-np.arange(half, dtype=np.float32) / np.float32(half))
    cos, sin = np.cos(angle), np.sin(angle)
    turn = jnp.asarray(np.stack([np.concatenate([cos, cos]), np.concatenate([-sin, sin])]).astype(np.float32))
    k, v = (c.reshape(SEQS, CACHE * KV, HEAD) for c in (k_cache, v_cache))
    vmem, dma = pltpu.VMEM, pltpu.SemaphoreType.DMA
    return pl.pallas_call(
        kernel,
        out_shape=jax.ShapeDtypeStruct((SEQS, D), BF16),
        in_specs=[pl.BlockSpec(memory_space=pl.ANY)] * 11,
        out_specs=pl.BlockSpec(memory_space=pl.ANY),
        scratch_shapes=[
            vmem((SEQS, D), BF16),
            vmem((1, D), BF16),
            vmem((1, D), BF16),
            vmem((2, HEAD), F32),
            vmem((RING, CACHE * KV, HEAD), BF16),
            vmem((RING, CACHE * KV, HEAD), BF16),
            vmem((2 * BLOCKS, HEADS * HEAD, COLS), BF16),
            vmem((FF_BLOCKS, D, COLS), BF16),
            vmem((FF_BLOCKS, D, COLS), BF16),
            vmem((2 * BLOCKS, FF, COLS), BF16),
            vmem((SEQS, 8, HEAD), F32),
            vmem((SEQS, 8, HEAD), F32),
            vmem((HEAD, CHUNK), F32),
            vmem((SEQS, D), BF16),
            vmem((SEQS, FF), BF16),
            vmem((SEQS, D), BF16),
            *[vmem((2, BLOCKS, SEQS, COLS), BF16)] * 4,
            dma((RING,)),
            dma((RING,)),
            dma((4,)),
            dma((2,)),
            dma((2 * BLOCKS,)),
            dma((FF_BLOCKS,)),
            dma((FF_BLOCKS,)),
            dma((2 * BLOCKS,)),
            dma((BLOCKS,)),
            dma((2, 3, BLOCKS)),
            dma((2, 3, BLOCKS)),
        ],
        compiler_params=pltpu.CompilerParams(collective_id=0, has_side_effects=True, vmem_limit_bytes=67_043_328),
    )(x, k, v, gain_a.reshape(1, D), wq, wo, gain_m.reshape(1, D), w_gate, w_up, w_down, turn)


def solution(mesh):
    states, cache, columns, rows_of = P("dp", None), P("dp", None, "tp", None), P(None, "tp"), P("tp", None)
    return jax.shard_map(
        layer,
        mesh=mesh,
        in_specs=(states, cache, cache, P(None), columns, rows_of, P(None), columns, columns, rows_of),
        out_specs=states,
        check_vma=False,
    )
```

```python
import functools

import jax
import jax.numpy as jnp
import numpy as np
from jax import lax
from jax.experimental import pallas as pl
from jax.experimental.pallas import tpu as pltpu
from jax.sharding import PartitionSpec as P

MESH = pl.DeviceIdType.MESH
BF16, F32 = jnp.bfloat16, jnp.float32
HEAD = 128
THETA = 10000
SEQS, CACHE, D, FF = 64, 4096, 3072, 2048
HEADS, KV = 6, 2
RING = 4
CHUNK = 512
COLS = 512
HALF = D // 2
BLOCKS = HALF // COLS
FF_BLOCKS = FF // COLS
EARLY = 48


def dot(a, w):
    return jnp.dot(a, w, preferred_element_type=F32)


def normed(x, gain):
    wide = x.astype(F32)
    scale = lax.rsqrt(jnp.mean(wide * wide, -1, keepdims=True) + 1e-6)
    return (wide * scale * gain.astype(F32).reshape(1, D)).astype(BF16)


def pair(ref, p, first, rows):
    at = 2 * p * CHUNK + first
    return jnp.concatenate([ref[at : at + rows, :], ref[at + CHUNK : at + CHUNK + rows, :]], 1)


def scores_of(k, q):
    zero = jnp.zeros((8, HEAD), F32)
    two = jnp.concatenate([jnp.concatenate([q, zero], 1), jnp.concatenate([zero, q], 1)], 0).astype(BF16)
    sums = [None, None]
    rows = CHUNK // 2
    for p in range(8):
        above, below = [jnp.zeros((n, 2 * HEAD), BF16) for n in (16 * p, 112 - 16 * p)]
        spread = jnp.concatenate([*([above] if p else []), two, *([below] if p < 7 else [])], 0)
        for h in range(2):
            term = lax.dot_general(pair(k, p, h * rows, rows), spread, (((1,), (1,)), ((), ())), preferred_element_type=F32)
            sums[h] = term if sums[h] is None else sums[h] + term
    return jnp.concatenate(sums, 0).T


def attended(scores, v, seen):
    s = scores.reshape(16, 8, CHUNK)
    s = jnp.where(seen, s, -jnp.inf)
    top = jnp.max(jnp.max(s, 0), 1, keepdims=True)
    e = jnp.exp2((s - top[None]) * (HEAD**-0.5 * 1.4426950408889634))
    total = jnp.sum(jnp.sum(e, 0), 1, keepdims=True)
    w = (e * (1.0 / total)[None]).reshape(128, CHUNK).astype(BF16)
    sums = [None, None]
    rows = CHUNK // 2
    for p in range(8):
        for h in range(2):
            term = dot(w[16 * p : 16 * p + 16, h * rows : h * rows + rows], pair(v, p, h * rows, rows))
            sums[h] = term if sums[h] is None else sums[h] + term
    both = sums[0] + sums[1]
    return both[:8, :HEAD] + both[8:, HEAD:]


def kernel(
    x_hbm, k_hbm, v_hbm, ga_hbm, wq_hbm, wo_hbm, gm_hbm, wg_hbm, wu_hbm, wd_hbm, turn_hbm,
    y_hbm,
    x, ga, gm, turn, kbuf, vbuf, wo, wg, wu, wd, q, o, scores, h, hidden, y,
    half_out, half_in, chip_out, chip_in,
    ksem, vsem, small_sem, wq_sem, wo_sem, wg_sem, wu_sem, wd_sem, y_sem, send_sem, recv_sem,
):
    me = lax.axis_index("tp")
    core = lax.rem(me, 2)
    partner = me + 1 - 2 * core
    across = lax.rem(me + 2, 4)
    own, other = core * HALF, (1 - core) * HALF

    def columns(start, i):
        return pl.ds(pl.multiple_of(start + i * COLS, COLS), COLS)

    small = [
        pltpu.make_async_copy(a, b, small_sem.at[i])
        for i, (a, b) in enumerate(((x_hbm, x), (ga_hbm, ga), (gm_hbm, gm), (turn_hbm, turn)))
    ]
    wq_copies = [
        pltpu.make_async_copy(wq_hbm.at[:, 0:512], wg.at[2], wq_sem.at[0]),
        pltpu.make_async_copy(wq_hbm.at[:, 512:768], wg.at[3, :, 0:256], wq_sem.at[1]),
    ]

    def k_copy(t):
        return pltpu.make_async_copy(k_hbm.at[t], kbuf.at[lax.rem(t, RING)], ksem.at[lax.rem(t, RING)])

    def v_copy(t):
        return pltpu.make_async_copy(v_hbm.at[t], vbuf.at[lax.rem(t, RING)], vsem.at[lax.rem(t, RING)])

    wo_copies, wd_copies = [
        [
            pltpu.make_async_copy(hbm.at[:, columns(other if i < BLOCKS else own, i % BLOCKS)], buf.at[i], sem.at[i])
            for i in range(2 * BLOCKS)
        ]
        for hbm, buf, sem in ((wo_hbm, wo, wo_sem), (wd_hbm, wd, wd_sem))
    ]
    wg_copies, wu_copies = [
        [pltpu.make_async_copy(hbm.at[:, i * COLS : (i + 1) * COLS], buf.at[i], sem.at[i]) for i in range(FF_BLOCKS)]
        for hbm, buf, sem in ((wg_hbm, wg, wg_sem), (wu_hbm, wu, wu_sem))
    ]

    def remote(which, phase, i, src, dst, device):
        return pltpu.make_async_remote_copy(
            src_ref=src, dst_ref=dst, send_sem=send_sem.at[which, phase, i], recv_sem=recv_sem.at[which, phase, i],
            device_id={"tp": device}, device_id_type=MESH,
        )

    class Sum:
        def __init__(self, which, at, first, rows, w, base, out, out_other):
            self.at, self.w, self.base, self.out, self.rows = at, w, base, out, pl.ds(first, rows)
            r = self.rows
            self.halves = [remote(which, 0, i, half_out.at[at, i, r], half_in.at[at, i, r], partner) for i in range(BLOCKS)]
            self.chips = [remote(which, 1, i, chip_out.at[at, i, r], chip_in.at[at, i, r], across) for i in range(BLOCKS)]
            self.finals = [
                remote(which, 2, i, out.at[r, columns(own, i)], out_other.at[r, columns(own, i)], partner) for i in range(BLOCKS)
            ]

        def swap_halves(self, lhs, ready=lambda i: None):
            for i in range(BLOCKS):
                ready(i)
                half_out[self.at, i, self.rows] = dot(lhs, self.w[i]).astype(BF16)
                self.halves[i].start()

        def swap_chips(self, lhs, ready=lambda i: None):
            for i in range(BLOCKS):
                ready(BLOCKS + i)
                term = dot(lhs, self.w[BLOCKS + i])
                self.halves[i].wait_recv()
                chip_out[self.at, i, self.rows] = (term + half_in[self.at, i, self.rows].astype(F32)).astype(BF16)
                self.chips[i].start()

        def swap_finals(self, keep=lambda i: None):
            for i in range(BLOCKS):
                self.chips[i].wait_recv()
                total = chip_out[self.at, i, self.rows].astype(F32) + chip_in[self.at, i, self.rows].astype(F32)
                cols = columns(own, i)
                self.out[self.rows, cols] = (self.base[self.rows, cols].astype(F32) + total).astype(BF16)
                self.finals[i].start()
                keep(i)

        def finish(self):
            for c in self.finals:
                c.wait()
            for c in (*self.halves, *self.chips):
                c.wait_send()

    for c in (*small, *wq_copies):
        c.start()
    for t in range(RING):
        k_copy(jnp.int32(t)).start()
        v_copy(jnp.int32(t)).start()
    for c in wo_copies:
        c.start()

    barrier = pltpu.get_barrier_semaphore()
    for d in (partner, across):
        pl.semaphore_signal(barrier, inc=1, device_id={"tp": d}, device_id_type=MESH)

    for c in small:
        c.wait()
    a = normed(x[...], ga[...])
    for c in wq_copies:
        c.wait()
    projected = jnp.concatenate([dot(a, wg[2]), dot(a, wg[3, :, 0:256])], 1).astype(BF16).astype(F32)
    cos, sin = turn[0:1, :], turn[1:2, :]
    for i in range(HEADS):
        t = projected[:, i * HEAD : (i + 1) * HEAD]
        q[:, i, :] = (t * cos + pltpu.roll(t, HEAD // 2, 1) * sin).astype(BF16).astype(F32)
    for i in range(HEADS, 8):
        q[:, i, :] = jnp.zeros((SEQS, HEAD), F32)

    row = lax.broadcasted_iota(jnp.int32, (8, CHUNK), 0)
    odd = lax.broadcasted_iota(jnp.int32, (8, CHUNK), 1) % 2
    seen = (((row < 3) & (odd == 0)) | ((row >= 3) & (row < 6) & (odd == 1)) | (row >= 6))[None]

    first = jnp.int32(0)
    k_copy(first).wait()
    scores[...] = scores_of(kbuf.at[0], q[0])
    k_copy(first + RING).start()

    def attention_of(first, rows):
        return jnp.concatenate([o[first : first + rows, i, :] for i in range(HEADS)], 1).astype(BF16)

    early, late = [Sum(which, 0, first, rows, wo, x, h, h) for which, first, rows in ((0, 0, EARLY), (1, EARLY, SEQS - EARLY))]

    def step(t, _):
        k_copy(t + 1).wait()
        v_copy(t).wait()
        before = scores[...]
        after = scores_of(kbuf.at[lax.rem(t + 1, RING)], q[t + 1])
        o[t] = attended(before, vbuf.at[lax.rem(t, RING)], seen)
        scores[...] = after

        @pl.when(t + RING < SEQS)
        def _():
            v_copy(t + RING).start()

            @pl.when(t + 1 + RING < SEQS)
            def _():
                k_copy(t + 1 + RING).start()

        @pl.when(t == SEQS - RING)
        def _():
            for c in (*(c for two in zip(wg_copies, wu_copies) for c in two), *wd_copies):
                c.start()

        @pl.when(t == EARLY)
        def _():
            pl.semaphore_wait(barrier, 2)
            for c in wo_copies:
                c.wait()
            early.swap_halves(attention_of(0, EARLY))

        @pl.when(t == EARLY + 2)
        def _():
            early.swap_chips(attention_of(0, EARLY))

        @pl.when(t == EARLY + 6)
        def _():
            early.swap_finals()

        @pl.when(t == EARLY + 9)
        def _():
            early.finish()
            y[:EARLY] = normed(h[:EARLY], gm[...])

        return 0

    lax.fori_loop(0, SEQS - 1, step, 0)
    last = jnp.int32(SEQS - 1)
    v_copy(last).wait()
    o[SEQS - 1] = attended(scores[...], vbuf.at[RING - 1], seen)


    attention = attention_of(EARLY, SEQS - EARLY)
    late.swap_halves(attention)
    late.swap_chips(attention)
    late.swap_finals()
    late.finish()
    y[EARLY:] = normed(h[EARLY:], gm[...])

    for i in range(FF_BLOCKS):
        wg_copies[i].wait()
        wu_copies[i].wait()
        gate = dot(y[...], wg[i])
        up = dot(y[...], wu[i])
        hidden[:, i * COLS : (i + 1) * COLS] = (gate * lax.logistic(gate) * up).astype(BF16)

    mlp = Sum(2, 1, 0, SEQS, wd, h, y, y_hbm)
    y_copies = [
        pltpu.make_async_copy(y.at[:, columns(own, i)], y_hbm.at[:, columns(own, i)], y_sem.at[i]) for i in range(BLOCKS)
    ]
    mlp.swap_halves(hidden[...], lambda i: wd_copies[i].wait())
    mlp.swap_chips(hidden[...], lambda i: wd_copies[i].wait())
    mlp.swap_finals(lambda i: y_copies[i].start())
    mlp.finish()
    for c in y_copies:
        c.wait()


def layer(x, k_cache, v_cache, gain_a, wq, wo, gain_m, w_gate, w_up, w_down):
    half = HEAD // 2
    angle = np.float32(CACHE - 1) * np.float32(THETA) ** (-np.arange(half, dtype=np.float32) / np.float32(half))
    cos, sin = np.cos(angle), np.sin(angle)
    turn = jnp.asarray(np.stack([np.concatenate([cos, cos]), np.concatenate([-sin, sin])]).astype(np.float32))
    k, v = (c.reshape(SEQS, CACHE * KV, HEAD) for c in (k_cache, v_cache))
    vmem, dma = pltpu.VMEM, pltpu.SemaphoreType.DMA
    return pl.pallas_call(
        kernel,
        out_shape=jax.ShapeDtypeStruct((SEQS, D), BF16),
        in_specs=[pl.BlockSpec(memory_space=pl.ANY)] * 11,
        out_specs=pl.BlockSpec(memory_space=pl.ANY),
        scratch_shapes=[
            vmem((SEQS, D), BF16),
            vmem((D,), BF16),
            vmem((D,), BF16),
            vmem((2, HEAD), F32),
            vmem((RING, CACHE * KV, HEAD), BF16),
            vmem((RING, CACHE * KV, HEAD), BF16),
            vmem((2 * BLOCKS, HEADS * HEAD, COLS), BF16),
            vmem((FF_BLOCKS, D, COLS), BF16),
            vmem((FF_BLOCKS, D, COLS), BF16),
            vmem((2 * BLOCKS, FF, COLS), BF16),
            vmem((SEQS, 8, HEAD), F32),
            vmem((SEQS, 8, HEAD), F32),
            vmem((HEAD, CHUNK), F32),
            vmem((SEQS, D), BF16),
            vmem((SEQS, FF), BF16),
            vmem((SEQS, D), BF16),
            *[vmem((2, BLOCKS, SEQS, COLS), BF16)] * 4,
            dma((RING,)),
            dma((RING,)),
            dma((4,)),
            dma((2,)),
            dma((2 * BLOCKS,)),
            dma((FF_BLOCKS,)),
            dma((FF_BLOCKS,)),
            dma((2 * BLOCKS,)),
            dma((BLOCKS,)),
            dma((3, 3, BLOCKS)),
            dma((3, 3, BLOCKS)),
        ],
        compiler_params=pltpu.CompilerParams(collective_id=0, has_side_effects=True, vmem_limit_bytes=67_043_328),
    )(x, k, v, gain_a, wq, wo, gain_m, w_gate, w_up, w_down, turn)


def solution(mesh):
    states, cache, columns, rows_of = P("dp", None), P("dp", None, "tp", None), P(None, "tp"), P("tp", None)
    return jax.shard_map(
        layer,
        mesh=mesh,
        in_specs=(states, cache, cache, P(None), columns, rows_of, P(None), columns, columns, rows_of),
        out_specs=states,
        check_vma=False,
    )
```

```python
import functools

import jax
import jax.numpy as jnp
import numpy as np
from jax import lax
from jax.experimental import pallas as pl
from jax.experimental.pallas import tpu as pltpu
from jax.sharding import PartitionSpec as P

MESH = pl.DeviceIdType.MESH
BF16, F32 = jnp.bfloat16, jnp.float32
HEAD = 128
THETA = 10000
SEQS, CACHE, D, FF = 64, 4096, 3072, 2048
HEADS, KV = 6, 2
RING = 4
CHUNK = 512
COLS = 512
HALF = D // 2
BLOCKS = HALF // COLS
FF_BLOCKS = FF // COLS
EARLY = 48


def dot(a, w):
    return jnp.dot(a, w, preferred_element_type=F32)


def normed(x, gain):
    wide = x.astype(F32)
    scale = lax.rsqrt(jnp.mean(wide * wide, -1, keepdims=True) + 1e-6)
    return (wide * scale * gain.astype(F32).reshape(1, D)).astype(BF16)


def pair(ref, p, first, rows):
    at = 2 * p * CHUNK + first
    return jnp.concatenate([ref[at : at + rows, :], ref[at + CHUNK : at + CHUNK + rows, :]], 1)


def scores_of(k, q):
    zero = jnp.zeros((8, HEAD), F32)
    two = jnp.concatenate([jnp.concatenate([q, zero], 1), jnp.concatenate([zero, q], 1)], 0).astype(BF16)
    sums = [None, None]
    rows = CHUNK // 2
    for p in range(8):
        above, below = [jnp.zeros((n, 2 * HEAD), BF16) for n in (16 * p, 112 - 16 * p)]
        spread = jnp.concatenate([*([above] if p else []), two, *([below] if p < 7 else [])], 0)
        for h in range(2):
            term = lax.dot_general(pair(k, p, h * rows, rows), spread, (((1,), (1,)), ((), ())), preferred_element_type=F32)
            sums[h] = term if sums[h] is None else sums[h] + term
    return jnp.concatenate(sums, 0).T


def attended(scores, v, seen):
    s = scores.reshape(16, 8, CHUNK)
    s = jnp.where(seen, s, -jnp.inf)
    top = jnp.max(jnp.max(s, 0), 1, keepdims=True)
    e = jnp.exp2((s - top[None]) * (HEAD**-0.5 * 1.4426950408889634))
    total = jnp.sum(jnp.sum(e, 0), 1, keepdims=True)
    w = (e * (1.0 / total)[None]).reshape(128, CHUNK).astype(BF16)
    sums = [None, None]
    rows = CHUNK // 2
    for p in range(8):
        for h in range(2):
            term = dot(w[16 * p : 16 * p + 16, h * rows : h * rows + rows], pair(v, p, h * rows, rows))
            sums[h] = term if sums[h] is None else sums[h] + term
    both = sums[0] + sums[1]
    return both[:8, :HEAD] + both[8:, HEAD:]


def kernel(
    x_hbm, k_hbm, v_hbm, ga_hbm, wq_hbm, wo_hbm, gm_hbm, wg_hbm, wu_hbm, wd_hbm, turn_hbm,
    y_hbm,
    x, ga, gm, turn, kbuf, vbuf, wo, wg, wu, wd, q, o, scores, attention, h, hidden, y,
    half_out, half_in, chip_out, chip_in,
    ksem, vsem, small_sem, wq_sem, wo_sem, wg_sem, wu_sem, wd_sem, y_sem, send_sem, recv_sem,
):
    me = lax.axis_index("tp")
    core = lax.rem(me, 2)
    partner = me + 1 - 2 * core
    across = lax.rem(me + 2, 4)
    own, other = core * HALF, (1 - core) * HALF

    def columns(start, i):
        return pl.ds(pl.multiple_of(start + i * COLS, COLS), COLS)

    small = [
        pltpu.make_async_copy(a, b, small_sem.at[i])
        for i, (a, b) in enumerate(((x_hbm, x), (ga_hbm, ga), (gm_hbm, gm), (turn_hbm, turn)))
    ]
    wq_copies = [
        pltpu.make_async_copy(wq_hbm.at[:, 0:512], wg.at[2], wq_sem.at[0]),
        pltpu.make_async_copy(wq_hbm.at[:, 512:768], wg.at[3, :, 0:256], wq_sem.at[1]),
    ]

    def k_copy(t):
        return pltpu.make_async_copy(k_hbm.at[t], kbuf.at[lax.rem(t, RING)], ksem.at[lax.rem(t, RING)])

    def v_copy(t):
        return pltpu.make_async_copy(v_hbm.at[t], vbuf.at[lax.rem(t, RING)], vsem.at[lax.rem(t, RING)])

    def block_copy(hbm, buf, sem):
        def copy(i):
            start = pl.multiple_of(jnp.where(i < BLOCKS, other, own) + lax.rem(i, BLOCKS) * COLS, COLS)
            return pltpu.make_async_copy(hbm.at[:, pl.ds(start, COLS)], buf.at[i], sem.at[i])

        return copy

    def ff_copy(hbm, buf, sem):
        def copy(i):
            return pltpu.make_async_copy(hbm.at[:, pl.ds(pl.multiple_of(i * COLS, COLS), COLS)], buf.at[i], sem.at[i])

        return copy

    wo_copy, wd_copy = block_copy(wo_hbm, wo, wo_sem), block_copy(wd_hbm, wd, wd_sem)
    wg_copy, wu_copy = ff_copy(wg_hbm, wg, wg_sem), ff_copy(wu_hbm, wu, wu_sem)

    def loop(n, body):
        def one(i, _):
            body(i)
            return 0

        lax.fori_loop(0, n, one, 0)

    class Sum:
        def __init__(self, which, at, first, rows, w, base, out, out_other):
            self.which, self.at, self.w, self.base, self.out, self.out_other = which, at, w, base, out, out_other
            self.rows = pl.ds(first, rows)

        def remote(self, phase, i, src, dst, device):
            return pltpu.make_async_remote_copy(
                src_ref=src, dst_ref=dst, send_sem=send_sem.at[self.which, phase, i], recv_sem=recv_sem.at[self.which, phase, i],
                device_id={"tp": device}, device_id_type=MESH,
            )

        def half(self, i):
            return self.remote(0, i, half_out.at[self.at, i, self.rows], half_in.at[self.at, i, self.rows], partner)

        def chip(self, i):
            return self.remote(1, i, chip_out.at[self.at, i, self.rows], chip_in.at[self.at, i, self.rows], across)

        def final(self, i):
            return self.remote(2, i, self.out.at[self.rows, columns(own, i)], self.out_other.at[self.rows, columns(own, i)], partner)

        def swap_halves(self, lhs, ready=lambda i: None):
            def body(i):
                ready(i)
                half_out[self.at, i, self.rows] = dot(lhs(), self.w[i]).astype(BF16)
                self.half(i).start()

            loop(BLOCKS, body)

        def swap_chips(self, lhs, ready=lambda i: None):
            def body(i):
                ready(BLOCKS + i)
                term = dot(lhs(), self.w[BLOCKS + i])
                self.half(i).wait_recv()
                chip_out[self.at, i, self.rows] = (term + half_in[self.at, i, self.rows].astype(F32)).astype(BF16)
                self.chip(i).start()

            loop(BLOCKS, body)

        def swap_finals(self, keep=lambda i: None):
            def body(i):
                self.chip(i).wait_recv()
                total = chip_out[self.at, i, self.rows].astype(F32) + chip_in[self.at, i, self.rows].astype(F32)
                cols = columns(own, i)
                self.out[self.rows, cols] = (self.base[self.rows, cols].astype(F32) + total).astype(BF16)
                self.final(i).start()
                keep(i)

            loop(BLOCKS, body)

        def finish(self):
            def body(i):
                self.final(i).wait()
                self.half(i).wait_send()
                self.chip(i).wait_send()

            loop(BLOCKS, body)

    for c in (*small, *wq_copies):
        c.start()
    for t in range(RING):
        k_copy(jnp.int32(t)).start()
        v_copy(jnp.int32(t)).start()
    loop(2 * BLOCKS, lambda i: wo_copy(i).start())

    barrier = pltpu.get_barrier_semaphore()
    for d in (partner, across):
        pl.semaphore_signal(barrier, inc=1, device_id={"tp": d}, device_id_type=MESH)

    for c in small:
        c.wait()
    a = normed(x[...], ga[...])
    for c in wq_copies:
        c.wait()
    projected = jnp.concatenate([dot(a, wg[2]), dot(a, wg[3, :, 0:256])], 1).astype(BF16).astype(F32)
    cos, sin = turn[0:1, :], turn[1:2, :]
    for i in range(HEADS):
        t = projected[:, i * HEAD : (i + 1) * HEAD]
        q[:, i, :] = (t * cos + pltpu.roll(t, HEAD // 2, 1) * sin).astype(BF16).astype(F32)
    for i in range(HEADS, 8):
        q[:, i, :] = jnp.zeros((SEQS, HEAD), F32)

    row = lax.broadcasted_iota(jnp.int32, (8, CHUNK), 0)
    odd = lax.broadcasted_iota(jnp.int32, (8, CHUNK), 1) % 2
    seen = (((row < 3) & (odd == 0)) | ((row >= 3) & (row < 6) & (odd == 1)) | (row >= 6))[None]

    first = jnp.int32(0)
    k_copy(first).wait()
    scores[...] = scores_of(kbuf.at[0], q[0])
    k_copy(first + RING).start()

    def attention_of(first, rows):
        return jnp.concatenate([o[first : first + rows, i, :] for i in range(HEADS)], 1).astype(BF16)

    early, late = [Sum(which, 0, first, rows, wo, x, h, h) for which, first, rows in ((0, 0, EARLY), (1, EARLY, SEQS - EARLY))]

    def step(t, _):
        @pl.when(t + 1 < SEQS)
        def _():
            k_copy(t + 1).wait()

        v_copy(t).wait()
        before = scores[...]
        after = scores_of(kbuf.at[lax.rem(t + 1, RING)], q[jnp.minimum(t + 1, SEQS - 1)])
        o[t] = attended(before, vbuf.at[lax.rem(t, RING)], seen)
        scores[...] = after

        @pl.when(t + RING < SEQS)
        def _():
            v_copy(t + RING).start()

            @pl.when(t + 1 + RING < SEQS)
            def _():
                k_copy(t + 1 + RING).start()

        @pl.when(t == SEQS - RING)
        def _():
            def both(i):
                wg_copy(i).start()
                wu_copy(i).start()

            loop(FF_BLOCKS, both)
            loop(2 * BLOCKS, lambda i: wd_copy(i).start())

        @pl.when(t == EARLY)
        def _():
            pl.semaphore_wait(barrier, 2)
            loop(2 * BLOCKS, lambda i: wo_copy(i).wait())
            attention[:EARLY] = attention_of(0, EARLY)
            early.swap_halves(lambda: attention[:EARLY])

        @pl.when(t == EARLY + 2)
        def _():
            early.swap_chips(lambda: attention[:EARLY])

        @pl.when(t == EARLY + 7)
        def _():
            early.swap_finals()

        @pl.when(t == EARLY + 10)
        def _():
            early.finish()

        return 0

    lax.fori_loop(0, SEQS, step, 0)

    attention[EARLY:] = attention_of(EARLY, SEQS - EARLY)
    late.swap_halves(lambda: attention[EARLY:])
    late.swap_chips(lambda: attention[EARLY:])
    y[:EARLY] = normed(h[:EARLY], gm[...])
    late.swap_finals()
    late.finish()
    y[EARLY:] = normed(h[EARLY:], gm[...])

    def ff(i):
        wg_copy(i).wait()
        wu_copy(i).wait()
        gate = dot(y[...], wg[i])
        up = dot(y[...], wu[i])
        hidden[:, pl.ds(pl.multiple_of(i * COLS, COLS), COLS)] = (gate * lax.logistic(gate) * up).astype(BF16)

    loop(FF_BLOCKS, ff)

    def y_copy(i):
        return pltpu.make_async_copy(y.at[:, columns(own, i)], y_hbm.at[:, columns(own, i)], y_sem.at[i])

    mlp = Sum(2, 1, 0, SEQS, wd, h, y, y_hbm)
    mlp.swap_halves(lambda: hidden[...], lambda i: wd_copy(i).wait())
    mlp.swap_chips(lambda: hidden[...], lambda i: wd_copy(i).wait())
    mlp.swap_finals(lambda i: y_copy(i).start())
    mlp.finish()
    loop(BLOCKS, lambda i: y_copy(i).wait())


def layer(x, k_cache, v_cache, gain_a, wq, wo, gain_m, w_gate, w_up, w_down):
    half = HEAD // 2
    angle = np.float32(CACHE - 1) * np.float32(THETA) ** (-np.arange(half, dtype=np.float32) / np.float32(half))
    cos, sin = np.cos(angle), np.sin(angle)
    turn = jnp.asarray(np.stack([np.concatenate([cos, cos]), np.concatenate([-sin, sin])]).astype(np.float32))
    k, v = (c.reshape(SEQS, CACHE * KV, HEAD) for c in (k_cache, v_cache))
    vmem, dma = pltpu.VMEM, pltpu.SemaphoreType.DMA
    return pl.pallas_call(
        kernel,
        out_shape=jax.ShapeDtypeStruct((SEQS, D), BF16),
        in_specs=[pl.BlockSpec(memory_space=pl.ANY)] * 11,
        out_specs=pl.BlockSpec(memory_space=pl.ANY),
        scratch_shapes=[
            vmem((SEQS, D), BF16),
            vmem((D,), BF16),
            vmem((D,), BF16),
            vmem((2, HEAD), F32),
            vmem((RING, CACHE * KV, HEAD), BF16),
            vmem((RING, CACHE * KV, HEAD), BF16),
            vmem((2 * BLOCKS, HEADS * HEAD, COLS), BF16),
            vmem((FF_BLOCKS, D, COLS), BF16),
            vmem((FF_BLOCKS, D, COLS), BF16),
            vmem((2 * BLOCKS, FF, COLS), BF16),
            vmem((SEQS, 8, HEAD), F32),
            vmem((SEQS, 8, HEAD), F32),
            vmem((HEAD, CHUNK), F32),
            vmem((SEQS, HEADS * HEAD), BF16),
            vmem((SEQS, D), BF16),
            vmem((SEQS, FF), BF16),
            vmem((SEQS, D), BF16),
            *[vmem((2, BLOCKS, SEQS, COLS), BF16)] * 4,
            dma((RING,)),
            dma((RING,)),
            dma((4,)),
            dma((2,)),
            dma((2 * BLOCKS,)),
            dma((FF_BLOCKS,)),
            dma((FF_BLOCKS,)),
            dma((2 * BLOCKS,)),
            dma((BLOCKS,)),
            dma((3, 3, BLOCKS)),
            dma((3, 3, BLOCKS)),
        ],
        compiler_params=pltpu.CompilerParams(collective_id=0, has_side_effects=True, vmem_limit_bytes=67_043_328),
    )(x, k, v, gain_a, wq, wo, gain_m, w_gate, w_up, w_down, turn)


def solution(mesh):
    states, cache, columns, rows_of = P("dp", None), P("dp", None, "tp", None), P(None, "tp"), P("tp", None)
    return jax.shard_map(
        layer,
        mesh=mesh,
        in_specs=(states, cache, cache, P(None), columns, rows_of, P(None), columns, columns, rows_of),
        out_specs=states,
        check_vma=False,
    )
```

```python
import functools

import jax
import jax.numpy as jnp
import numpy as np
from jax import lax
from jax.experimental import pallas as pl
from jax.experimental.pallas import tpu as pltpu
from jax.sharding import PartitionSpec as P

MESH = pl.DeviceIdType.MESH
BF16, F32 = jnp.bfloat16, jnp.float32
HEAD = 128
THETA = 10000
SEQS, CACHE, D, FF = 64, 4096, 3072, 2048
HEADS, KV = 6, 2
RING = 4
CHUNK = 512
COLS = 512
HALF = D // 2
BLOCKS = HALF // COLS
FF_BLOCKS = FF // COLS
EARLY = 48


def dot(a, w):
    return jnp.dot(a, w, preferred_element_type=F32)


def normed(x, gain):
    wide = x.astype(F32)
    scale = lax.rsqrt(jnp.mean(wide * wide, -1, keepdims=True) + 1e-6)
    return (wide * scale * gain.astype(F32).reshape(1, D)).astype(BF16)


def pair(ref, p, first, rows):
    at = 2 * p * CHUNK + first
    return jnp.concatenate([ref[at : at + rows, :], ref[at + CHUNK : at + CHUNK + rows, :]], 1)


def scores_of(k, q):
    zero = jnp.zeros((8, HEAD), F32)
    two = jnp.concatenate([jnp.concatenate([q, zero], 1), jnp.concatenate([zero, q], 1)], 0).astype(BF16)
    sums = [None, None]
    rows = CHUNK // 2
    for p in range(8):
        above, below = [jnp.zeros((n, 2 * HEAD), BF16) for n in (16 * p, 112 - 16 * p)]
        spread = jnp.concatenate([*([above] if p else []), two, *([below] if p < 7 else [])], 0)
        for h in range(2):
            term = lax.dot_general(pair(k, p, h * rows, rows), spread, (((1,), (1,)), ((), ())), preferred_element_type=F32)
            sums[h] = term if sums[h] is None else sums[h] + term
    return jnp.concatenate(sums, 0).T


def attended(scores, v, seen):
    s = scores.reshape(16, 8, CHUNK)
    s = jnp.where(seen, s, -jnp.inf)
    top = jnp.max(jnp.max(s, 0), 1, keepdims=True)
    e = jnp.exp2((s - top[None]) * (HEAD**-0.5 * 1.4426950408889634))
    total = jnp.sum(jnp.sum(e, 0), 1, keepdims=True)
    w = (e * (1.0 / total)[None]).reshape(128, CHUNK).astype(BF16)
    sums = [None, None]
    rows = CHUNK // 2
    for p in range(8):
        for h in range(2):
            term = dot(w[16 * p : 16 * p + 16, h * rows : h * rows + rows], pair(v, p, h * rows, rows))
            sums[h] = term if sums[h] is None else sums[h] + term
    both = sums[0] + sums[1]
    return both[:8, :HEAD] + both[8:, HEAD:]


def kernel(
    x_hbm, k_hbm, v_hbm, ga_hbm, wq_hbm, wo_hbm, gm_hbm, wg_hbm, wu_hbm, wd_hbm, turn_hbm,
    y_hbm,
    x, ga, gm, turn, kbuf, vbuf, wo, wg, wu, wd, q, o, scores, attention, h, hidden, y,
    half_out, half_in, chip_out, chip_in,
    ksem, vsem, small_sem, wq_sem, wo_sem, wg_sem, wu_sem, wd_sem, y_sem, send_sem, recv_sem,
):
    me = lax.axis_index("tp")
    core = lax.rem(me, 2)
    partner = me + 1 - 2 * core
    across = lax.rem(me + 2, 4)
    own, other = core * HALF, (1 - core) * HALF

    def columns(start, i):
        return pl.ds(pl.multiple_of(start + i * COLS, COLS), COLS)

    small = [
        pltpu.make_async_copy(a, b, small_sem.at[i])
        for i, (a, b) in enumerate(((x_hbm, x), (ga_hbm, ga), (gm_hbm, gm), (turn_hbm, turn)))
    ]
    wq_copies = [
        pltpu.make_async_copy(wq_hbm.at[:, 0:512], wg.at[2], wq_sem.at[0]),
        pltpu.make_async_copy(wq_hbm.at[:, 512:768], wg.at[3, :, 0:256], wq_sem.at[1]),
    ]

    def k_copy(t):
        return pltpu.make_async_copy(k_hbm.at[t], kbuf.at[lax.rem(t, RING)], ksem.at[lax.rem(t, RING)])

    def v_copy(t):
        return pltpu.make_async_copy(v_hbm.at[t], vbuf.at[lax.rem(t, RING)], vsem.at[lax.rem(t, RING)])

    def block_copy(hbm, buf, sem):
        def copy(i):
            start = pl.multiple_of(jnp.where(i < BLOCKS, other, own) + lax.rem(i, BLOCKS) * COLS, COLS)
            return pltpu.make_async_copy(hbm.at[:, pl.ds(start, COLS)], buf.at[i], sem.at[i])

        return copy

    def ff_copy(hbm, buf, sem):
        def copy(i):
            return pltpu.make_async_copy(hbm.at[:, pl.ds(pl.multiple_of(i * COLS, COLS), COLS)], buf.at[i], sem.at[i])

        return copy

    wo_copy, wd_copy = block_copy(wo_hbm, wo, wo_sem), block_copy(wd_hbm, wd, wd_sem)
    wg_copy, wu_copy = ff_copy(wg_hbm, wg, wg_sem), ff_copy(wu_hbm, wu, wu_sem)

    def loop(n, body):
        def one(i, _):
            body(i)
            return 0

        lax.fori_loop(0, n, one, 0)

    class Sum:
        def __init__(self, which, at, first, rows, w, base, out, out_other):
            self.which, self.at, self.w, self.base, self.out, self.out_other = which, at, w, base, out, out_other
            self.rows = pl.ds(first, rows)

        def remote(self, phase, i, src, dst, device):
            return pltpu.make_async_remote_copy(
                src_ref=src, dst_ref=dst, send_sem=send_sem.at[self.which, phase, i], recv_sem=recv_sem.at[self.which, phase, i],
                device_id={"tp": device}, device_id_type=MESH,
            )

        def half(self, i):
            return self.remote(0, i, half_out.at[self.at, i, self.rows], half_in.at[self.at, i, self.rows], partner)

        def chip(self, i):
            return self.remote(1, i, chip_out.at[self.at, i, self.rows], chip_in.at[self.at, i, self.rows], across)

        def final(self, i):
            return self.remote(2, i, self.out.at[self.rows, columns(own, i)], self.out_other.at[self.rows, columns(own, i)], partner)

        def swap_halves(self, lhs, ready=lambda i: None):
            def body(i):
                ready(i)
                half_out[self.at, i, self.rows] = dot(lhs(), self.w[i]).astype(BF16)
                self.half(i).start()

            loop(BLOCKS, body)

        def swap_chips(self, lhs, ready=lambda i: None):
            def body(i):
                ready(BLOCKS + i)
                term = dot(lhs(), self.w[BLOCKS + i])
                self.half(i).wait_recv()
                chip_out[self.at, i, self.rows] = (term + half_in[self.at, i, self.rows].astype(F32)).astype(BF16)
                self.chip(i).start()

            loop(BLOCKS, body)

        def swap_finals(self, keep=lambda i: None):
            def body(i):
                self.chip(i).wait_recv()
                total = chip_out[self.at, i, self.rows].astype(F32) + chip_in[self.at, i, self.rows].astype(F32)
                cols = columns(own, i)
                self.out[self.rows, cols] = (self.base[self.rows, cols].astype(F32) + total).astype(BF16)
                self.final(i).start()
                keep(i)

            loop(BLOCKS, body)

        def finish(self):
            def body(i):
                self.final(i).wait()
                self.half(i).wait_send()
                self.chip(i).wait_send()

            loop(BLOCKS, body)

    for c in (*small, *wq_copies):
        c.start()
    for t in range(1):
        k_copy(jnp.int32(t)).start()
        v_copy(jnp.int32(t)).start()

    barrier = pltpu.get_barrier_semaphore()
    for d in (partner, across):
        pl.semaphore_signal(barrier, inc=1, device_id={"tp": d}, device_id_type=MESH)

    for c in small:
        c.wait()
    a = normed(x[...], ga[...])
    for c in wq_copies:
        c.wait()
    for t in range(1, RING):
        k_copy(jnp.int32(t)).start()
        v_copy(jnp.int32(t)).start()
    loop(2 * BLOCKS, lambda i: wo_copy(i).start())
    projected = jnp.concatenate([dot(a, wg[2]), dot(a, wg[3, :, 0:256])], 1).astype(BF16).astype(F32)
    cos, sin = turn[0:1, :], turn[1:2, :]
    for i in range(HEADS):
        t = projected[:, i * HEAD : (i + 1) * HEAD]
        q[:, i, :] = (t * cos + pltpu.roll(t, HEAD // 2, 1) * sin).astype(BF16).astype(F32)
    for i in range(HEADS, 8):
        q[:, i, :] = jnp.zeros((SEQS, HEAD), F32)

    row = lax.broadcasted_iota(jnp.int32, (8, CHUNK), 0)
    odd = lax.broadcasted_iota(jnp.int32, (8, CHUNK), 1) % 2
    seen = (((row < 3) & (odd == 0)) | ((row >= 3) & (row < 6) & (odd == 1)) | (row >= 6))[None]

    first = jnp.int32(0)
    k_copy(first).wait()
    scores[...] = scores_of(kbuf.at[0], q[0])
    k_copy(first + RING).start()

    def attention_of(first, rows):
        return jnp.concatenate([o[first : first + rows, i, :] for i in range(HEADS)], 1).astype(BF16)

    early, late = [Sum(which, 0, first, rows, wo, x, h, h) for which, first, rows in ((0, 0, EARLY), (1, EARLY, SEQS - EARLY))]

    def step(t, _):
        @pl.when(t + 1 < SEQS)
        def _():
            k_copy(t + 1).wait()

        v_copy(t).wait()
        before = scores[...]
        after = scores_of(kbuf.at[lax.rem(t + 1, RING)], q[jnp.minimum(t + 1, SEQS - 1)])
        o[t] = attended(before, vbuf.at[lax.rem(t, RING)], seen)
        scores[...] = after

        @pl.when(t + RING < SEQS)
        def _():
            v_copy(t + RING).start()

            @pl.when(t + 1 + RING < SEQS)
            def _():
                k_copy(t + 1 + RING).start()

        @pl.when(t == SEQS - RING)
        def _():
            def both(i):
                wg_copy(i).start()
                wu_copy(i).start()

            loop(FF_BLOCKS, both)
            loop(2 * BLOCKS, lambda i: wd_copy(i).start())

        @pl.when(t == EARLY)
        def _():
            pl.semaphore_wait(barrier, 2)
            loop(2 * BLOCKS, lambda i: wo_copy(i).wait())
            attention[:EARLY] = attention_of(0, EARLY)
            early.swap_halves(lambda: attention[:EARLY])

        @pl.when(t == EARLY + 2)
        def _():
            early.swap_chips(lambda: attention[:EARLY])

        @pl.when(t == EARLY + 7)
        def _():
            early.swap_finals()

        @pl.when(t == EARLY + 10)
        def _():
            early.finish()

        return 0

    lax.fori_loop(0, SEQS, step, 0)

    attention[EARLY:] = attention_of(EARLY, SEQS - EARLY)
    late.swap_halves(lambda: attention[EARLY:])
    late.swap_chips(lambda: attention[EARLY:])
    y[:EARLY] = normed(h[:EARLY], gm[...])
    late.swap_finals()
    late.finish()
    y[EARLY:] = normed(h[EARLY:], gm[...])

    def ff(i):
        wg_copy(i).wait()
        wu_copy(i).wait()
        gate = dot(y[...], wg[i])
        up = dot(y[...], wu[i])
        hidden[:, pl.ds(pl.multiple_of(i * COLS, COLS), COLS)] = (gate * lax.logistic(gate) * up).astype(BF16)

    loop(FF_BLOCKS, ff)

    def y_copy(i):
        return pltpu.make_async_copy(y.at[:, columns(own, i)], y_hbm.at[:, columns(own, i)], y_sem.at[i])

    mlp = Sum(2, 1, 0, SEQS, wd, h, y, y_hbm)
    mlp.swap_halves(lambda: hidden[...], lambda i: wd_copy(i).wait())
    mlp.swap_chips(lambda: hidden[...], lambda i: wd_copy(i).wait())
    mlp.swap_finals(lambda i: y_copy(i).start())
    mlp.finish()
    loop(BLOCKS, lambda i: y_copy(i).wait())


def layer(x, k_cache, v_cache, gain_a, wq, wo, gain_m, w_gate, w_up, w_down):
    half = HEAD // 2
    angle = np.float32(CACHE - 1) * np.float32(THETA) ** (-np.arange(half, dtype=np.float32) / np.float32(half))
    cos, sin = np.cos(angle), np.sin(angle)
    turn = jnp.asarray(np.stack([np.concatenate([cos, cos]), np.concatenate([-sin, sin])]).astype(np.float32))
    k, v = (c.reshape(SEQS, CACHE * KV, HEAD) for c in (k_cache, v_cache))
    vmem, dma = pltpu.VMEM, pltpu.SemaphoreType.DMA
    return pl.pallas_call(
        kernel,
        out_shape=jax.ShapeDtypeStruct((SEQS, D), BF16),
        in_specs=[pl.BlockSpec(memory_space=pl.ANY)] * 11,
        out_specs=pl.BlockSpec(memory_space=pl.ANY),
        scratch_shapes=[
            vmem((SEQS, D), BF16),
            vmem((D,), BF16),
            vmem((D,), BF16),
            vmem((2, HEAD), F32),
            vmem((RING, CACHE * KV, HEAD), BF16),
            vmem((RING, CACHE * KV, HEAD), BF16),
            vmem((2 * BLOCKS, HEADS * HEAD, COLS), BF16),
            vmem((FF_BLOCKS, D, COLS), BF16),
            vmem((FF_BLOCKS, D, COLS), BF16),
            vmem((2 * BLOCKS, FF, COLS), BF16),
            vmem((SEQS, 8, HEAD), F32),
            vmem((SEQS, 8, HEAD), F32),
            vmem((HEAD, CHUNK), F32),
            vmem((SEQS, HEADS * HEAD), BF16),
            vmem((SEQS, D), BF16),
            vmem((SEQS, FF), BF16),
            vmem((SEQS, D), BF16),
            *[vmem((2, BLOCKS, SEQS, COLS), BF16)] * 4,
            dma((RING,)),
            dma((RING,)),
            dma((4,)),
            dma((2,)),
            dma((2 * BLOCKS,)),
            dma((FF_BLOCKS,)),
            dma((FF_BLOCKS,)),
            dma((2 * BLOCKS,)),
            dma((BLOCKS,)),
            dma((3, 3, BLOCKS)),
            dma((3, 3, BLOCKS)),
        ],
        compiler_params=pltpu.CompilerParams(collective_id=0, has_side_effects=True, vmem_limit_bytes=67_043_328),
    )(x, k, v, gain_a, wq, wo, gain_m, w_gate, w_up, w_down, turn)


def solution(mesh):
    states, cache, columns, rows_of = P("dp", None), P("dp", None, "tp", None), P(None, "tp"), P("tp", None)
    return jax.shard_map(
        layer,
        mesh=mesh,
        in_specs=(states, cache, cache, P(None), columns, rows_of, P(None), columns, columns, rows_of),
        out_specs=states,
        check_vma=False,
    )
```

```python
import functools

import jax
import jax.numpy as jnp
import numpy as np
from jax import lax
from jax.experimental import pallas as pl
from jax.experimental.pallas import tpu as pltpu
from jax.sharding import PartitionSpec as P

MESH = pl.DeviceIdType.MESH
BF16, F32 = jnp.bfloat16, jnp.float32
HEAD = 128
THETA = 10000
SEQS, CACHE, D, FF = 64, 4096, 3072, 2048
HEADS, KV = 6, 2
RING = 4
CHUNK = 512
COLS = 512
HALF = D // 2
BLOCKS = HALF // COLS
FF_BLOCKS = FF // COLS
EARLY = 48


def dot(a, w):
    return jnp.dot(a, w, preferred_element_type=F32)


def normed(x, gain):
    wide = x.astype(F32)
    scale = lax.rsqrt(jnp.mean(wide * wide, -1, keepdims=True) + 1e-6)
    return (wide * scale * gain.astype(F32).reshape(1, D)).astype(BF16)


def pair(ref, p, first, rows):
    at = 2 * p * CHUNK + first
    return jnp.concatenate([ref[at : at + rows, :], ref[at + CHUNK : at + CHUNK + rows, :]], 1)


def scores_of(k, q):
    zero = jnp.zeros((8, HEAD), F32)
    two = jnp.concatenate([jnp.concatenate([q, zero], 1), jnp.concatenate([zero, q], 1)], 0).astype(BF16)
    sums = [None, None]
    rows = CHUNK // 2
    for p in range(8):
        above, below = [jnp.zeros((n, 2 * HEAD), BF16) for n in (16 * p, 112 - 16 * p)]
        spread = jnp.concatenate([*([above] if p else []), two, *([below] if p < 7 else [])], 0)
        for h in range(2):
            term = lax.dot_general(pair(k, p, h * rows, rows), spread, (((1,), (1,)), ((), ())), preferred_element_type=F32)
            sums[h] = term if sums[h] is None else sums[h] + term
    return jnp.concatenate(sums, 0).T


def attended(scores, v, seen):
    s = scores.reshape(16, 8, CHUNK)
    s = jnp.where(seen, s, -jnp.inf)
    top = jnp.max(jnp.max(s, 0), 1, keepdims=True)
    e = jnp.exp2((s - top[None]) * (HEAD**-0.5 * 1.4426950408889634))
    total = jnp.sum(jnp.sum(e, 0), 1, keepdims=True)
    w = (e * (1.0 / total)[None]).reshape(128, CHUNK).astype(BF16)
    sums = [None, None]
    rows = CHUNK // 2
    for p in range(8):
        for h in range(2):
            term = dot(w[16 * p : 16 * p + 16, h * rows : h * rows + rows], pair(v, p, h * rows, rows))
            sums[h] = term if sums[h] is None else sums[h] + term
    both = sums[0] + sums[1]
    return both[:8, :HEAD] + both[8:, HEAD:]


def kernel(
    x_hbm, k_hbm, v_hbm, ga_hbm, wq_hbm, wo_hbm, gm_hbm, wg_hbm, wu_hbm, wd_hbm, turn_hbm,
    y_hbm,
    x, ga, gm, turn, kbuf, vbuf, wo, wg, wu, wd, q, o, scores, attention, h, hidden, y,
    half_out, half_in, chip_out, chip_in,
    ksem, vsem, small_sem, wq_sem, wo_sem, wg_sem, wu_sem, wd_sem, y_sem, send_sem, recv_sem,
):
    me = lax.axis_index("tp")
    core = lax.rem(me, 2)
    partner = me + 1 - 2 * core
    across = lax.rem(me + 2, 4)
    own, other = core * HALF, (1 - core) * HALF

    def columns(start, i):
        return pl.ds(pl.multiple_of(start + i * COLS, COLS), COLS)

    small = [
        pltpu.make_async_copy(a, b, small_sem.at[i])
        for i, (a, b) in enumerate(((x_hbm, x), (ga_hbm, ga), (gm_hbm, gm), (turn_hbm, turn)))
    ]
    wq_copies = [
        pltpu.make_async_copy(wq_hbm.at[:, 0:512], wg.at[2], wq_sem.at[0]),
        pltpu.make_async_copy(wq_hbm.at[:, 512:768], wg.at[3, :, 0:256], wq_sem.at[1]),
    ]

    def k_copy(t):
        return pltpu.make_async_copy(k_hbm.at[t], kbuf.at[lax.rem(t, RING)], ksem.at[lax.rem(t, RING)])

    def v_copy(t):
        return pltpu.make_async_copy(v_hbm.at[t], vbuf.at[lax.rem(t, RING)], vsem.at[lax.rem(t, RING)])

    def block_copy(hbm, buf, sem):
        def copy(i):
            start = pl.multiple_of(jnp.where(i < BLOCKS, other, own) + lax.rem(i, BLOCKS) * COLS, COLS)
            return pltpu.make_async_copy(hbm.at[:, pl.ds(start, COLS)], buf.at[i], sem.at[i])

        return copy

    def ff_copy(hbm, buf, sem):
        def copy(i):
            return pltpu.make_async_copy(hbm.at[:, pl.ds(pl.multiple_of(i * COLS, COLS), COLS)], buf.at[i], sem.at[i])

        return copy

    wo_copy, wd_copy = block_copy(wo_hbm, wo, wo_sem), block_copy(wd_hbm, wd, wd_sem)
    wg_copy, wu_copy = ff_copy(wg_hbm, wg, wg_sem), ff_copy(wu_hbm, wu, wu_sem)

    def loop(n, body):
        def one(i, _):
            body(i)
            return 0

        lax.fori_loop(0, n, one, 0)

    class Sum:
        def __init__(self, which, at, first, rows, w, base, out, out_other):
            self.which, self.at, self.w, self.base, self.out, self.out_other = which, at, w, base, out, out_other
            self.rows = pl.ds(first, rows)

        def remote(self, phase, i, src, dst, device):
            return pltpu.make_async_remote_copy(
                src_ref=src, dst_ref=dst, send_sem=send_sem.at[self.which, phase, i], recv_sem=recv_sem.at[self.which, phase, i],
                device_id={"tp": device}, device_id_type=MESH,
            )

        def half(self, i):
            return self.remote(0, i, half_out.at[self.at, i, self.rows], half_in.at[self.at, i, self.rows], partner)

        def chip(self, i):
            return self.remote(1, i, chip_out.at[self.at, i, self.rows], chip_in.at[self.at, i, self.rows], across)

        def final(self, i):
            return self.remote(2, i, self.out.at[self.rows, columns(own, i)], self.out_other.at[self.rows, columns(own, i)], partner)

        def swap_halves(self, lhs, ready=lambda i: None):
            def body(i):
                ready(i)
                half_out[self.at, i, self.rows] = dot(lhs(), self.w[i]).astype(BF16)
                self.half(i).start()

            loop(BLOCKS, body)

        def swap_chips(self, lhs, ready=lambda i: None):
            def body(i):
                ready(BLOCKS + i)
                term = dot(lhs(), self.w[BLOCKS + i])
                self.half(i).wait_recv()
                chip_out[self.at, i, self.rows] = (term + half_in[self.at, i, self.rows].astype(F32)).astype(BF16)
                self.chip(i).start()

            loop(BLOCKS, body)

        def swap_finals(self, keep=lambda i: None):
            def body(i):
                self.chip(i).wait_recv()
                total = chip_out[self.at, i, self.rows].astype(F32) + chip_in[self.at, i, self.rows].astype(F32)
                cols = columns(own, i)
                self.out[self.rows, cols] = (self.base[self.rows, cols].astype(F32) + total).astype(BF16)
                self.final(i).start()
                keep(i)

            loop(BLOCKS, body)

        def finish(self):
            def body(i):
                self.final(i).wait()
                self.half(i).wait_send()
                self.chip(i).wait_send()

            loop(BLOCKS, body)

    for c in (*small, *wq_copies):
        c.start()
    for t in range(1):
        k_copy(jnp.int32(t)).start()
        v_copy(jnp.int32(t)).start()

    barrier = pltpu.get_barrier_semaphore()
    for d in (partner, across):
        pl.semaphore_signal(barrier, inc=1, device_id={"tp": d}, device_id_type=MESH)

    for c in small:
        c.wait()
    a = normed(x[...], ga[...])
    for c in wq_copies:
        c.wait()
    for t in range(1, RING):
        k_copy(jnp.int32(t)).start()
        v_copy(jnp.int32(t)).start()
    loop(2 * BLOCKS, lambda i: wo_copy(i).start())
    projected = jnp.concatenate([dot(a, wg[2]), dot(a, wg[3, :, 0:256])], 1).astype(BF16).astype(F32)
    cos, sin = turn[0:1, :], turn[1:2, :]
    for i in range(HEADS):
        t = projected[:, i * HEAD : (i + 1) * HEAD]
        q[:, i, :] = (t * cos + pltpu.roll(t, HEAD // 2, 1) * sin).astype(BF16).astype(F32)
    for i in range(HEADS, 8):
        q[:, i, :] = jnp.zeros((SEQS, HEAD), F32)

    row = lax.broadcasted_iota(jnp.int32, (8, CHUNK), 0)
    odd = lax.broadcasted_iota(jnp.int32, (8, CHUNK), 1) % 2
    seen = (((row < 3) & (odd == 0)) | ((row >= 3) & (row < 6) & (odd == 1)) | (row >= 6))[None]

    first = jnp.int32(0)
    k_copy(first).wait()
    scores[...] = scores_of(kbuf.at[0], q[0])
    k_copy(first + RING).start()

    def attention_of(first, rows):
        return jnp.concatenate([o[first : first + rows, i, :] for i in range(HEADS)], 1).astype(BF16)

    early, late = [Sum(which, 0, first, rows, wo, x, h, h) for which, first, rows in ((0, 0, EARLY), (1, EARLY, SEQS - EARLY))]

    def step(t, _):
        @pl.when(t + 1 < SEQS)
        def _():
            k_copy(t + 1).wait()

        v_copy(t).wait()
        before = scores[...]
        after = scores_of(kbuf.at[lax.rem(t + 1, RING)], q[jnp.minimum(t + 1, SEQS - 1)])
        o[t] = attended(before, vbuf.at[lax.rem(t, RING)], seen)
        scores[...] = after

        @pl.when(t + RING < SEQS)
        def _():
            v_copy(t + RING).start()

            @pl.when(t + 1 + RING < SEQS)
            def _():
                k_copy(t + 1 + RING).start()

        @pl.when(t == SEQS - RING)
        def _():
            def both(i):
                wg_copy(i).start(priority=1)
                wu_copy(i).start(priority=1)

            loop(FF_BLOCKS, both)
            loop(2 * BLOCKS, lambda i: wd_copy(i).start(priority=1))

        @pl.when(t == EARLY)
        def _():
            pl.semaphore_wait(barrier, 2)
            loop(2 * BLOCKS, lambda i: wo_copy(i).wait())
            attention[:EARLY] = attention_of(0, EARLY)
            early.swap_halves(lambda: attention[:EARLY])

        @pl.when(t == EARLY + 2)
        def _():
            early.swap_chips(lambda: attention[:EARLY])

        @pl.when(t == EARLY + 7)
        def _():
            early.swap_finals()

        @pl.when(t == EARLY + 10)
        def _():
            early.finish()

        return 0

    lax.fori_loop(0, SEQS, step, 0)

    attention[EARLY:] = attention_of(EARLY, SEQS - EARLY)
    late.swap_halves(lambda: attention[EARLY:])
    late.swap_chips(lambda: attention[EARLY:])
    y[:EARLY] = normed(h[:EARLY], gm[...])
    late.swap_finals()
    late.finish()
    y[EARLY:] = normed(h[EARLY:], gm[...])

    def ff(i):
        wg_copy(i).wait()
        wu_copy(i).wait()
        gate = dot(y[...], wg[i])
        up = dot(y[...], wu[i])
        hidden[:, pl.ds(pl.multiple_of(i * COLS, COLS), COLS)] = (gate * lax.logistic(gate) * up).astype(BF16)

    loop(FF_BLOCKS, ff)

    def y_copy(i):
        return pltpu.make_async_copy(y.at[:, columns(own, i)], y_hbm.at[:, columns(own, i)], y_sem.at[i])

    mlp = Sum(2, 1, 0, SEQS, wd, h, y, y_hbm)
    mlp.swap_halves(lambda: hidden[...], lambda i: wd_copy(i).wait())
    mlp.swap_chips(lambda: hidden[...], lambda i: wd_copy(i).wait())
    mlp.swap_finals(lambda i: y_copy(i).start())
    mlp.finish()
    loop(BLOCKS, lambda i: y_copy(i).wait())


def layer(x, k_cache, v_cache, gain_a, wq, wo, gain_m, w_gate, w_up, w_down):
    half = HEAD // 2
    angle = np.float32(CACHE - 1) * np.float32(THETA) ** (-np.arange(half, dtype=np.float32) / np.float32(half))
    cos, sin = np.cos(angle), np.sin(angle)
    turn = jnp.asarray(np.stack([np.concatenate([cos, cos]), np.concatenate([-sin, sin])]).astype(np.float32))
    k, v = (c.reshape(SEQS, CACHE * KV, HEAD) for c in (k_cache, v_cache))
    vmem, dma = pltpu.VMEM, pltpu.SemaphoreType.DMA
    return pl.pallas_call(
        kernel,
        out_shape=jax.ShapeDtypeStruct((SEQS, D), BF16),
        in_specs=[pl.BlockSpec(memory_space=pl.ANY)] * 11,
        out_specs=pl.BlockSpec(memory_space=pl.ANY),
        scratch_shapes=[
            vmem((SEQS, D), BF16),
            vmem((D,), BF16),
            vmem((D,), BF16),
            vmem((2, HEAD), F32),
            vmem((RING, CACHE * KV, HEAD), BF16),
            vmem((RING, CACHE * KV, HEAD), BF16),
            vmem((2 * BLOCKS, HEADS * HEAD, COLS), BF16),
            vmem((FF_BLOCKS, D, COLS), BF16),
            vmem((FF_BLOCKS, D, COLS), BF16),
            vmem((2 * BLOCKS, FF, COLS), BF16),
            vmem((SEQS, 8, HEAD), F32),
            vmem((SEQS, 8, HEAD), F32),
            vmem((HEAD, CHUNK), F32),
            vmem((SEQS, HEADS * HEAD), BF16),
            vmem((SEQS, D), BF16),
            vmem((SEQS, FF), BF16),
            vmem((SEQS, D), BF16),
            *[vmem((2, BLOCKS, SEQS, COLS), BF16)] * 4,
            dma((RING,)),
            dma((RING,)),
            dma((4,)),
            dma((2,)),
            dma((2 * BLOCKS,)),
            dma((FF_BLOCKS,)),
            dma((FF_BLOCKS,)),
            dma((2 * BLOCKS,)),
            dma((BLOCKS,)),
            dma((3, 3, BLOCKS)),
            dma((3, 3, BLOCKS)),
        ],
        compiler_params=pltpu.CompilerParams(collective_id=0, has_side_effects=True, vmem_limit_bytes=67_043_328),
    )(x, k, v, gain_a, wq, wo, gain_m, w_gate, w_up, w_down, turn)


def solution(mesh):
    states, cache, columns, rows_of = P("dp", None), P("dp", None, "tp", None), P(None, "tp"), P("tp", None)
    return jax.shard_map(
        layer,
        mesh=mesh,
        in_specs=(states, cache, cache, P(None), columns, rows_of, P(None), columns, columns, rows_of),
        out_specs=states,
        check_vma=False,
    )
```
